8 devices in a mesh: dp: 1 (over z), sp: 8 (over x, y, core).
Axes of the slice: x: 2, y: 2, z: 1, core: 2. Of those that a mesh axis runs over, the one named last changes fastest.
Arguments:
- x: bfloat16 [2048, 12288], P(('dp', 'sp'))
- gain: bfloat16 [12288], replicated
- wq: bfloat16 [12288, 12288], replicated
- wk: bfloat16 [12288, 1024], replicated
- wv: bfloat16 [12288, 1024], replicated
- wo: bfloat16 [12288, 12288], replicated
Outputs:
- output: bfloat16 [2048, 12288], P(('dp', 'sp'))
All inputs are finite; a program needn't handle non-finite values.
Results may differ from the reference program's by a relative error of at most 0.012.
Values are sent between devices in bfloat16 or wider.
A program may use at most 2 GiB of HBM per device.

```python
import jax
import jax.numpy as jnp
from jax import lax

ROWS = 2048
D = 12288
HEADS = 96
KV_HEADS = 8
HEAD = 128
THETA = 10000


def setup_inputs(seed: int = 0, part: int = 0) -> dict:
    kx, kn, kq, kk, kv, ko = jax.random.split(jax.random.key(seed), 6)

    def weights(key, rows, columns):
        return jax.random.normal(key, (rows, columns), jnp.float32) * rows**-0.5

    drawn = {
        "x": jax.random.normal(jax.random.fold_in(kx, part), (ROWS, D), jnp.float32),
        "gain": 1 + 0.1 * jax.random.normal(kn, (D,), jnp.float32),
        "wq": 2 * weights(kq, D, HEADS * HEAD),
        "wk": 2 * weights(kk, D, KV_HEADS * HEAD),
        "wv": 4 * weights(kv, D, KV_HEADS * HEAD),
        "wo": weights(ko, HEADS * HEAD, D),
    }
    return {k: v.astype(jnp.bfloat16) for k, v in drawn.items()}


def normed(x, gain):
    wide = x.astype(jnp.float32)
    scale = lax.rsqrt(jnp.mean(wide * wide, -1, keepdims=True) + 1e-6)
    return (wide * scale * gain.astype(jnp.float32)).astype(jnp.bfloat16)


def turned(t, place, theta):
    half = t.shape[-1] // 2
    angle = place.astype(jnp.float32)[:, None] * theta ** (-jnp.arange(half, dtype=jnp.float32) / half)
    cos, sin = jnp.cos(angle)[:, None], jnp.sin(angle)[:, None]
    a, b = t[..., :half].astype(jnp.float32), t[..., half:].astype(jnp.float32)
    return jnp.concatenate([a * cos - b * sin, b * cos + a * sin], -1).astype(jnp.bfloat16)


def matmul(a, w):
    return jnp.dot(a, w, preferred_element_type=jnp.float32).astype(jnp.bfloat16)


def einsum(form, a, b):
    return jnp.einsum(form, a.astype(jnp.float32), b.astype(jnp.float32))


def attention(q, k, v):
    scores = einsum("tgsd,ugd->gstu", q, k) * q.shape[-1] ** -0.5
    token = jnp.arange(q.shape[0])
    scores = jnp.where(token[:, None] >= token, scores, -jnp.inf)
    weights = jax.nn.softmax(scores, -1).astype(jnp.bfloat16)
    return einsum("gstu,ugd->tgsd", weights, v).astype(jnp.bfloat16)


def reference(x, gain, wq, wk, wv, wo):
    a, place = normed(x, gain), jnp.arange(ROWS)
    q = turned(matmul(a, wq).reshape(ROWS, HEADS, HEAD), place, THETA).reshape(ROWS, KV_HEADS, -1, HEAD)
    k = turned(matmul(a, wk).reshape(ROWS, KV_HEADS, HEAD), place, THETA)
    v = matmul(a, wv).reshape(ROWS, KV_HEADS, HEAD)
    seen = attention(q, k, v).reshape(ROWS, HEADS * HEAD)
    return (x.astype(jnp.float32) + jnp.dot(seen, wo, preferred_element_type=jnp.float32)).astype(jnp.bfloat16)
```

```python
import functools

import jax
import jax.numpy as jnp
from jax import lax
from jax.experimental import pallas as pl
from jax.experimental.pallas import tpu as pltpu
from jax.sharding import PartitionSpec as P

HEAD = 128
THETA = 10000
NEG = -1e30
HIDDEN = 2 * NEG
LOG2E = 1.4426950408889634
TN = 512
CHUNKS = 4


def _dot(a, b, ca, cb):
    return lax.dot_general(a, b, (((ca,), (cb,)), ((), ())), preferred_element_type=jnp.float32)


def _project(chips, x_ref, gain_ref, cos_ref, sin_ref, wq_ref, wk_ref, wv_ref, q_ref, k_ref, v_ref,
             a_s, w_s, o_s, x_sem, a_send, a_recv, w_sem, q_sem, kv_send, kv_recv, kv_own):
    me = lax.axis_index("sp")
    core = lax.rem(me, 2)
    chip = lax.div(me, 2)
    partner = me + 1 - 2 * core
    own, depth = x_ref.shape
    rows = own // CHUNKS
    heads = TN // HEAD
    tiles = q_ref.shape[0] // heads

    x_in = [pltpu.make_async_copy(x_ref.at[pl.ds(i * rows, rows)], a_s.at[core, pl.ds(i * rows, rows)], x_sem.at[i]) for i in range(CHUNKS)]
    for c in x_in:
        c.start()

    def weights(ref, at, slot):
        return pltpu.make_async_copy(ref.at[:, pl.ds(pl.multiple_of(at, TN), TN)], w_s.at[slot], w_sem.at[slot])

    weights(wk_ref, core * TN, 0).start()
    weights(wv_ref, core * TN, 1).start()
    weights(wq_ref, core * tiles * TN, 2).start()

    others = [lax.rem(chip + i, chips) * 2 + core for i in range(1, chips)]
    barrier = pltpu.get_barrier_semaphore()
    for d in [partner, *others]:
        pl.semaphore_signal(barrier, inc=1, device_id={"sp": d}, device_id_type=pl.DeviceIdType.MESH)
    pl.semaphore_wait(barrier, len(others) + 1)

    def share(i):
        part = a_s.at[core, pl.ds(i * rows, rows)]
        return pltpu.make_async_remote_copy(part, part, a_send.at[i], a_recv.at[i], device_id={"sp": partner}, device_id_type=pl.DeviceIdType.MESH)

    step = 16

    def norm(i, _):
        here = pl.ds(pl.multiple_of(i * step, step), step)
        wide = a_s[core, here, :].astype(jnp.float32)
        scale = lax.rsqrt(jnp.mean(wide * wide, -1, keepdims=True) + 1e-6)
        a_s[core, here, :] = (wide * scale * gain_ref[...]).astype(jnp.bfloat16)

    for i in range(CHUNKS):
        x_in[i].wait()
        lax.fori_loop(i * rows // step, (i + 1) * rows // step, norm, None)
        share(i).start()

    def arrived(i):
        part = a_s.at[1 - core, pl.ds(i * rows, rows)]
        return pltpu.make_async_remote_copy(part, part, a_send.at[i], a_recv.at[i], device_id={"sp": partner}, device_id_type=pl.DeviceIdType.MESH)

    def put(t):
        slot = 2 + lax.rem(t, 2)
        return pltpu.make_async_copy(o_s.at[slot], q_ref.at[pl.ds(t * heads, heads)], q_sem.at[slot - 2])

    def spread(i, kind):
        out = (k_ref, v_ref)[kind].at[:, pl.ds(pl.multiple_of(chip * 2 * own, 2 * own), 2 * own), :]
        return pltpu.make_async_remote_copy(o_s.at[kind], out, kv_send.at[kind, i], kv_recv.at[kind, i],
                                            device_id={"sp": others[i]}, device_id_type=pl.DeviceIdType.MESH)

    def keep(kind):
        out = (k_ref, v_ref)[kind].at[:, pl.ds(pl.multiple_of(chip * 2 * own, 2 * own), 2 * own), :]
        return pltpu.make_async_copy(o_s.at[kind], out, kv_own.at[kind])

    def job(j, _):
        first = j < 4
        t = lax.div(j - 4, 2)
        half = jnp.where(first, jnp.where(j < 2, core, 1 - core), lax.rem(j, 2))
        slot = jnp.where(first, lax.rem(j, 2), lax.rem(2 + t, 3))
        entry = jnp.where(first, lax.rem(j, 2), 2 + lax.rem(t, 2))
        turn = lax.rem(j, 2) == 0
        turn = turn | jnp.logical_not(first)

        @pl.when(j < 2)
        def _():
            weights(wk_ref, 0, slot).wait()

        @pl.when(j == 2)
        def _():
            for i in range(CHUNKS):
                arrived(i).wait_recv()

        @pl.when(jnp.logical_not(first) & (lax.rem(j, 2) == 0))
        def _():
            weights(wq_ref, 0, slot).wait()

            @pl.when(t >= 2)
            def _():
                put(t - 2).wait()

        acc = _dot(a_s[half], w_s[slot], 1, 0)
        at = pl.ds(pl.multiple_of(half * own, own), own)
        cos = jnp.where(turn, cos_ref[at, :], 1.0)
        sin = jnp.where(turn, sin_ref[at, :], 0.0)
        for h in range(heads):
            one = acc[:, h * HEAD : (h + 1) * HEAD].astype(jnp.bfloat16).astype(jnp.float32)
            o_s[entry, h, at, :] = (one * cos + pltpu.roll(one, HEAD // 2, 1) * sin).astype(jnp.bfloat16)

        @pl.when((j == 2) | (j == 3))
        def _():
            weights(wq_ref, (core * tiles + j - 1) * TN, slot).start()

        @pl.when(j == 3)
        def _():
            for kind in range(2):
                keep(kind).start()
                for i in range(len(others)):
                    spread(i, kind).start()

        @pl.when(jnp.logical_not(first) & (lax.rem(j, 2) == 1))
        def _():
            put(t).start()

            @pl.when(t + 3 < tiles)
            def _():
                weights(wq_ref, (core * tiles + t + 3) * TN, slot).start()

    lax.fori_loop(0, 4 + 2 * tiles, job, None)
    put(tiles - 2).wait()
    put(tiles - 1).wait()
    for i in range(CHUNKS):
        share(i).wait_send()
    for kind in range(2):
        keep(kind).wait()
        for i in range(len(others)):
            spread(i, kind).wait()


def project(x, gain, cos, sin, wq, wk, wv, chips):
    own, depth = x.shape
    heads, kv = wq.shape[1] // HEAD // 2, wk.shape[1] // HEAD // 2
    hbm, vmem = pl.BlockSpec(memory_space=pl.ANY), pl.BlockSpec(memory_space=pltpu.VMEM)
    keys = jax.ShapeDtypeStruct((kv, chips * 2 * own, HEAD), jnp.bfloat16)
    return pl.pallas_call(
        functools.partial(_project, chips),
        in_specs=[hbm, vmem, vmem, vmem, hbm, hbm, hbm],
        out_specs=[hbm, hbm, hbm],
        out_shape=[jax.ShapeDtypeStruct((heads, 2 * own, HEAD), jnp.bfloat16), keys, keys],
        scratch_shapes=[
            pltpu.VMEM((2, own, depth), jnp.bfloat16),
            pltpu.VMEM((3, depth, TN), jnp.bfloat16),
            pltpu.VMEM((4, TN // HEAD, 2 * own, HEAD), jnp.bfloat16),
            pltpu.SemaphoreType.DMA((CHUNKS,)),
            pltpu.SemaphoreType.DMA((CHUNKS,)),
            pltpu.SemaphoreType.DMA((CHUNKS,)),
            pltpu.SemaphoreType.DMA((3,)),
            pltpu.SemaphoreType.DMA((2,)),
            pltpu.SemaphoreType.DMA((2, chips - 1)),
            pltpu.SemaphoreType.DMA((2, chips - 1)),
            pltpu.SemaphoreType.DMA((2,)),
        ],
        compiler_params=pltpu.CompilerParams(collective_id=0, has_side_effects=True, vmem_limit_bytes=62 * 2**20),
    )(x, gain, cos, sin, wq, wk, wv)


def _forward(pos_ref, q_ref, k_ref, v_ref, o_ref, top_s, mix_s, *, scale, bk, wide):
    g, bq, d = q_ref.shape
    low = k_ref.dtype
    cols = g * bq
    e = scale * LOG2E
    pieces = list(range(0, cols, wide))
    start = pos_ref[1]
    top_s[...] = jnp.full((1, cols), NEG, jnp.float32)
    mix_s[...] = jnp.zeros((d + 8, cols), jnp.float32)
    ones = jnp.ones((8, bk), low)

    def block(j, masked):
        here = pl.ds(pl.multiple_of(j * bk, bk), bk)
        k = k_ref[0, here, :]
        scores = [_dot(k, q_ref[...].reshape(cols, d)[at : at + wide, :], 1, 1) for at in pieces]
        if masked:
            gap = lax.rem(lax.broadcasted_iota(jnp.int32, (bk, wide), 1), bq) - lax.broadcasted_iota(jnp.int32, (bk, wide), 0)
            ok = gap >= j * bk - start
        weights, keeps = [], []
        for at, s in zip(pieces, scores):
            if masked:
                s = jnp.where(ok, s, HIDDEN)
            old = top_s[:, at : at + wide]
            top = jnp.maximum(old, s.max(axis=0, keepdims=True))
            top_s[:, at : at + wide] = top
            weights.append(jnp.exp2((s - top) * e).astype(low))
            keeps.append(jnp.exp2((old - top) * e))
        values = jnp.concatenate([v_ref[0, here, :].T, ones], axis=0)
        for at, p, keep in zip(pieces, weights, keeps):
            mix_s[:, at : at + wide] = mix_s[:, at : at + wide] * keep + _dot(values, p, 1, 0)

    whole = lax.div(start + 1, bk)
    last = lax.div(start + bq - 1 + bk, bk)
    lax.fori_loop(0, whole, lambda j, _: block(j, False), None)
    lax.fori_loop(whole, last, lambda j, _: block(j, True), None)
    for n in range(g):
        at = n * bq
        o_ref[:, n * d : (n + 1) * d] = (mix_s[:d, at : at + bq] * (1 / mix_s[d : d + 1, at : at + bq])).T.astype(o_ref.dtype)


def attend(q, k, v, half, start, bq):
    h, _, d = q.shape
    kv, sk, _ = k.shape
    g = h // kv
    bk, wide = 512, 512
    return pl.pallas_call(
        functools.partial(_forward, scale=d**-0.5, bk=bk, wide=wide),
        grid_spec=pltpu.PrefetchScalarGridSpec(
            num_scalar_prefetch=1,
            grid=(kv,),
            in_specs=[
                pl.BlockSpec((g, bq, d), lambda i, pos: (i, pos[0], 0)),
                pl.BlockSpec((1, sk, d), lambda i, pos: (i, 0, 0)),
                pl.BlockSpec((1, sk, d), lambda i, pos: (i, 0, 0)),
            ],
            out_specs=pl.BlockSpec((bq, g * d), lambda i, pos: (0, i)),
            scratch_shapes=[pltpu.VMEM((1, g * bq), jnp.float32), pltpu.VMEM((d + 8, g * bq), jnp.float32)],
        ),
        out_shape=jax.ShapeDtypeStruct((bq, h * d), q.dtype),
        compiler_params=pltpu.CompilerParams(dimension_semantics=("arbitrary",), vmem_limit_bytes=56 * 2**20),
        cost_estimate=pl.CostEstimate(flops=4 * h * bq * sk * d, transcendentals=h * bq * sk, bytes_accessed=2 * (h * bq * d * 2 + 2 * kv * sk * d)),
    )(jnp.stack([half, start]).astype(jnp.int32), q, k, v)


def _out(x_ref, a_ref, b_ref, w_ref, y_ref):
    core = lax.rem(lax.axis_index("sp"), 2)
    depth = a_ref.shape[1]
    mine = w_ref[pl.ds(pl.multiple_of(core * depth, depth), depth), :]
    theirs = w_ref[pl.ds(pl.multiple_of((1 - core) * depth, depth), depth), :]
    y = _dot(a_ref[...], mine, 1, 0) + _dot(b_ref[...], theirs, 1, 0)
    y_ref[...] = (x_ref[...].astype(jnp.float32) + y).astype(y_ref.dtype)


def out_project(x, a, b, w):
    own, depth = a.shape
    n = w.shape[1]
    tn = 512
    return pl.pallas_call(
        _out,
        grid=(n // tn,),
        in_specs=[
            pl.BlockSpec((own, tn), lambda j: (0, j)),
            pl.BlockSpec((own, depth), lambda j: (0, 0), pipeline_mode=pl.Buffered(1)),
            pl.BlockSpec((own, depth), lambda j: (0, 0), pipeline_mode=pl.Buffered(1)),
            pl.BlockSpec((2 * depth, tn), lambda j: (0, j)),
        ],
        out_specs=pl.BlockSpec((own, tn), lambda j: (0, j)),
        out_shape=jax.ShapeDtypeStruct((own, n), x.dtype),
        compiler_params=pltpu.CompilerParams(dimension_semantics=("arbitrary",), vmem_limit_bytes=62 * 2**20),
        cost_estimate=pl.CostEstimate(flops=4 * own * depth * n, transcendentals=0, bytes_accessed=4 * depth * n),
    )(x, a, b, w)


def solution(mesh):
    devices = mesh.shape["sp"]

    def step(x, gain, wq, wk, wv, wo):
        own = x.shape[0]
        me = lax.axis_index("sp")
        core, first = me % 2, (me // 2) * 2 * own
        half = HEAD // 2
        angle = (first + jnp.arange(2 * own)).astype(jnp.float32)[:, None] * THETA ** (-jnp.arange(half, dtype=jnp.float32) / half)
        cos, sin = jnp.cos(angle), jnp.sin(angle)
        q, k, v = project(x, gain.astype(jnp.float32)[None], jnp.concatenate([cos, cos], -1), jnp.concatenate([-sin, sin], -1), wq, wk, wv, devices // 2)
        theirs = attend(q, k, v, 1 - core, first + (1 - core) * own, own)
        swapped = lax.ppermute(theirs, "sp", [(i, i ^ 1) for i in range(devices)])
        mine = attend(q, k, v, core, first + core * own, own)
        return out_project(x, mine, swapped, wo)

    tokens, whole = P(("dp", "sp"), None), P(None, None)
    return jax.shard_map(step, mesh=mesh, in_specs=(tokens, P(None), whole, whole, whole, whole), out_specs=tokens, check_vma=False)
```

```python
import functools

import jax
import jax.numpy as jnp
from jax import lax
from jax.experimental import pallas as pl
from jax.experimental.pallas import tpu as pltpu
from jax.sharding import PartitionSpec as P

HEAD = 128
THETA = 10000
NEG = -1e30
HIDDEN = 2 * NEG
LOG2E = 1.4426950408889634
TN = 512
CHUNKS = 4
RUN = 6
WIDE = 512
MESH = pl.DeviceIdType.MESH


def _dot(a, b, ca, cb):
    return lax.dot_general(a, b, (((ca,), (cb,)), ((), ())), preferred_element_type=jnp.float32)


def _layer(chips, x_ref, gain_ref, cos_ref, sin_ref, wq_ref, wk_ref, wv_ref, wo_ref, y_ref, q_ref, far_ref,
           a_s, w_s, o_s, kv_s, qb_s, top_s, mix_s, xs_s, ys_s,
           x_sem, a_send, a_recv, far_send, far_recv, w_sem, q_sem, kv_send, kv_recv, qb_sem, free_sem, s_send, s_recv, xs_sem, y_sem, y_send, y_recv):
    me = lax.axis_index("sp")
    core = lax.rem(me, 2)
    chip = lax.div(me, 2)
    partner = me + 1 - 2 * core
    own, depth = x_ref.shape
    rows = own // CHUNKS
    heads = TN // HEAD
    tiles = depth // 2 // TN
    others = [lax.rem(chip + i, chips) * 2 + core for i in range(1, chips)]

    def remote(src, dst, send, recv, device):
        return pltpu.make_async_remote_copy(src, dst, send, recv, device_id={"sp": device}, device_id_type=MESH)

    def columns(n, i):
        return pl.ds(pl.multiple_of(i * n, n), n)

    x_in = [pltpu.make_async_copy(x_ref.at[pl.ds(i * rows, rows)], a_s.at[core, pl.ds(i * rows, rows)], x_sem.at[i]) for i in range(CHUNKS)]
    for c in x_in:
        c.start()

    def weights(ref, i, slot):
        return pltpu.make_async_copy(ref.at[:, columns(TN, i)], w_s.at[slot], w_sem.at[slot])

    weights(wk_ref, core, 0).start()
    weights(wv_ref, core, 1).start()
    weights(wq_ref, core * tiles, 2).start()

    barrier = pltpu.get_barrier_semaphore()
    for d in [partner, *others]:
        pl.semaphore_signal(barrier, inc=1, device_id={"sp": d}, device_id_type=MESH)
    pl.semaphore_wait(barrier, len(others) + 1)

    def share(i, half):
        part = a_s.at[half, pl.ds(i * rows, rows)]
        return remote(part, part, a_send.at[i], a_recv.at[i], partner)

    step = 16

    def norm(i, _):
        here = pl.ds(pl.multiple_of(i * step, step), step)
        wide = a_s[core, here, :].astype(jnp.float32)
        scale = lax.rsqrt(jnp.mean(wide * wide, -1, keepdims=True) + 1e-6)
        a_s[core, here, :] = (wide * scale * gain_ref[...]).astype(jnp.bfloat16)

    for i in range(CHUNKS):
        x_in[i].wait()
        lax.fori_loop(i * rows // step, (i + 1) * rows // step, norm, None)
        share(i, core).start()

    far = remote(x_ref.at[:, columns(depth // 2, 1 - core)], far_ref, far_send, far_recv, partner)
    far.start()

    def put(t):
        slot = lax.rem(t, 2)
        return pltpu.make_async_copy(o_s.at[slot], q_ref.at[pl.ds(t * heads, heads)], q_sem.at[slot])

    def spread(i, kind):
        part = kv_s.at[kind, :, columns(2 * own, chip), :]
        return remote(part, part, kv_send.at[kind, i], kv_recv.at[kind, i], others[i])

    def job(j, _):
        first = j < 4
        t = lax.div(j - 4, 2)
        even = lax.rem(j, 2) == 0
        half = jnp.where(first, jnp.where(j < 2, core, 1 - core), lax.rem(j, 2))
        slot = jnp.where(first, lax.rem(j, 2), lax.rem(2 + t, 3))
        turn = even | jnp.logical_not(first)

        @pl.when(j < 2)
        def _():
            weights(wk_ref, 0, slot).wait()

        @pl.when(j == 2)
        def _():
            for i in range(CHUNKS):
                share(i, 1 - core).wait_recv()

        @pl.when(jnp.logical_not(first) & even)
        def _():
            weights(wq_ref, 0, slot).wait()

            @pl.when(t >= 2)
            def _():
                put(t - 2).wait()

        acc = _dot(a_s[half], w_s[slot], 1, 0)
        at = columns(own, half)
        cos = jnp.where(turn, cos_ref[at, :], 1.0)
        sin = jnp.where(turn, sin_ref[at, :], 0.0)
        turned = []
        for h in range(heads):
            one = acc[:, h * HEAD : (h + 1) * HEAD].astype(jnp.bfloat16).astype(jnp.float32)
            turned.append((one * cos + pltpu.roll(one, HEAD // 2, 1) * sin).astype(jnp.bfloat16))

        @pl.when(first)
        def _():
            for h in range(heads):
                kv_s[lax.rem(j, 2), h, columns(own, chip * 2 + half), :] = turned[h]

        @pl.when(jnp.logical_not(first))
        def _():
            for h in range(heads):
                o_s[lax.rem(t, 2), h, at, :] = turned[h]

        @pl.when((j == 2) | (j == 3))
        def _():
            weights(wq_ref, core * tiles + j - 1, slot).start()

        @pl.when(j == 3)
        def _():
            for kind in range(2):
                for i in range(len(others)):
                    spread(i, kind).start()

        @pl.when(jnp.logical_not(first) & jnp.logical_not(even))
        def _():
            put(t).start()

            @pl.when(t + 3 < tiles)
            def _():
                weights(wq_ref, core * tiles + t + 3, slot).start()

            @pl.when(t + 3 >= tiles)
            def _():
                weights(wo_ref, core * tiles + t + 3 - tiles, slot).start()

    lax.fori_loop(0, 4 + 2 * tiles, job, None)
    for i in range(CHUNKS):
        share(i, core).wait_send()
    pl.semaphore_signal(free_sem, inc=1, device_id={"sp": partner}, device_id_type=MESH)
    put(tiles - 2).wait()
    put(tiles - 1).wait()
    for kind in range(2):
        for i in range(len(others)):
            spread(i, kind).wait()

    runs = q_ref.shape[0] // RUN
    groups = kv_s.shape[1]
    cols = RUN * own
    e = HEAD**-0.5 * LOG2E
    pieces = list(range(0, cols, WIDE))

    def queries(r):
        slot = lax.rem(r, 2)
        return pltpu.make_async_copy(q_ref.at[pl.ds(lax.div(r, 2) * RUN, RUN), columns(own, lax.rem(r, 2))], qb_s.at[slot], qb_sem.at[slot])

    def seen(r):
        part = a_s.at[lax.rem(r, 2), :, columns(RUN * HEAD, core * runs + lax.div(r, 2))]
        return remote(part, part, s_send.at[r], s_recv.at[r], partner)

    def seen_in(r):
        part = a_s.at[lax.rem(r, 2), :, columns(RUN * HEAD, (1 - core) * runs + lax.div(r, 2))]
        return remote(part, part, s_send.at[r], s_recv.at[r], partner)

    queries(0).start()
    pl.semaphore_wait(free_sem, 1)

    def attend(r, _):
        slot = lax.rem(r, 2)
        group = lax.div(r, 2 * runs // groups)
        queries(r).wait()

        @pl.when(r + 1 < 2 * runs)
        def _():
            queries(r + 1).start()

        top_s[...] = jnp.full((1, cols), NEG, jnp.float32)
        mix_s[...] = jnp.zeros((HEAD + 8, cols), jnp.float32)

        def block(at, bk, masked):
            here = pl.ds(pl.multiple_of(at, bk), bk)
            k = kv_s[0, group, here, :]
            scores = [_dot(k, qb_s[slot].reshape(cols, HEAD)[p : p + WIDE, :], 1, 1) for p in pieces]
            if masked:
                ok = lax.rem(lax.broadcasted_iota(jnp.int32, (bk, WIDE), 1), own) >= lax.broadcasted_iota(jnp.int32, (bk, WIDE), 0)
            weights, keeps = [], []
            for p, s in zip(pieces, scores):
                if masked:
                    s = jnp.where(ok, s, HIDDEN)
                old = top_s[:, p : p + WIDE]
                top = jnp.maximum(old, s.max(axis=0, keepdims=True))
                top_s[:, p : p + WIDE] = top
                weights.append(jnp.exp2((s - top) * e).astype(jnp.bfloat16))
                keeps.append(jnp.exp2((old - top) * e))
            values = jnp.concatenate([kv_s[1, group, here, :].T, jnp.ones((8, bk), jnp.bfloat16)], axis=0)
            for p, w, keep in zip(pieces, weights, keeps):
                mix_s[:, p : p + WIDE] = mix_s[:, p : p + WIDE] * keep + _dot(values, w, 1, 0)

        lax.fori_loop(0, chip, lambda i, _: block(i * 2 * own, 2 * own, False), None)

        @pl.when(slot == 1)
        def _():
            block(chip * 2 * own, own, False)

        block((chip * 2 + slot) * own, own, True)
        for n in range(RUN):
            p = n * own
            one = (mix_s[:HEAD, p : p + own] * (1 / mix_s[HEAD : HEAD + 1, p : p + own])).T
            a_s[slot, :, columns(HEAD, (core * runs + lax.div(r, 2)) * RUN + n)] = one.astype(jnp.bfloat16)
        seen(r).start()

    lax.fori_loop(0, 2 * runs, attend, None)
    for r in range(2 * runs):
        seen_in(r).wait_recv()
    far.wait()

    def residual(t, u):
        part = (far_ref.at[:, columns(TN, t)], x_ref.at[:, columns(TN, core * tiles + t)])[u]
        return pltpu.make_async_copy(part, xs_s.at[u], xs_sem.at[u])

    def give(t):
        return remote(ys_s.at[0], y_ref.at[:, columns(TN, core * tiles + t)], y_send.at[t], y_recv.at[t], partner)

    def take(t):
        return remote(ys_s.at[0], y_ref.at[:, columns(TN, (1 - core) * tiles + t)], y_send.at[t], y_recv.at[t], partner)

    def store(t):
        return pltpu.make_async_copy(ys_s.at[1], y_ref.at[:, columns(TN, core * tiles + t)], y_sem)

    residual(0, 0).start()
    residual(0, 1).start()

    def out(j, _):
        u = lax.rem(j, 2)
        t = lax.div(j, 2)
        half = jnp.where(u == 0, 1 - core, core)
        slot = lax.rem(2 + tiles + t, 3)

        @pl.when(u == 0)
        def _():
            weights(wo_ref, 0, slot).wait()

        acc = _dot(a_s[half], w_s[slot], 1, 0)

        @pl.when(u == 0)
        def _():
            residual(t, 0).wait()

            @pl.when(t > 0)
            def _():
                give(t - 1).wait_send()

        @pl.when(u == 1)
        def _():
            residual(t, 1).wait()

            @pl.when(t > 0)
            def _():
                store(t - 1).wait()

        ys_s[u] = (xs_s[u].astype(jnp.float32) + acc).astype(jnp.bfloat16)

        @pl.when(u == 0)
        def _():
            give(t).start()

            @pl.when(t + 1 < tiles)
            def _():
                residual(t + 1, 0).start()

        @pl.when(u == 1)
        def _():
            store(t).start()

            @pl.when(t + 1 < tiles)
            def _():
                residual(t + 1, 1).start()

            @pl.when(t + 3 < tiles)
            def _():
                weights(wo_ref, core * tiles + t + 3, slot).start()

    lax.fori_loop(0, 2 * tiles, out, None)
    for r in range(2 * runs):
        seen(r).wait_send()
    give(tiles - 1).wait_send()
    store(tiles - 1).wait()
    for t in range(tiles):
        take(t).wait_recv()


def layer(x, gain, cos, sin, wq, wk, wv, wo, chips):
    own, depth = x.shape
    heads, kv = wq.shape[1] // HEAD // 2, wk.shape[1] // HEAD // 2
    tiles, runs = depth // 2 // TN, heads // RUN
    hbm, vmem = pl.BlockSpec(memory_space=pl.ANY), pl.BlockSpec(memory_space=pltpu.VMEM)
    low, dma = jnp.bfloat16, pltpu.SemaphoreType.DMA
    y, _, _ = pl.pallas_call(
        functools.partial(_layer, chips),
        in_specs=[hbm, vmem, vmem, vmem, hbm, hbm, hbm, hbm],
        out_specs=[hbm, hbm, hbm],
        out_shape=[jax.ShapeDtypeStruct((own, depth), low), jax.ShapeDtypeStruct((heads, 2 * own, HEAD), low), jax.ShapeDtypeStruct((own, depth // 2), low)],
        scratch_shapes=[
            pltpu.VMEM((2, own, depth), low),
            pltpu.VMEM((3, depth, TN), low),
            pltpu.VMEM((2, TN // HEAD, 2 * own, HEAD), low),
            pltpu.VMEM((2, kv, chips * 2 * own, HEAD), low),
            pltpu.VMEM((2, RUN, own, HEAD), low),
            pltpu.VMEM((1, RUN * own), jnp.float32),
            pltpu.VMEM((HEAD + 8, RUN * own), jnp.float32),
            pltpu.VMEM((2, own, TN), low),
            pltpu.VMEM((2, own, TN), low),
            dma((CHUNKS,)), dma((CHUNKS,)), dma((CHUNKS,)), dma, dma, dma((3,)), dma((2,)), dma((2, chips - 1)), dma((2, chips - 1)),
            dma((2,)), pltpu.SemaphoreType.REGULAR, dma((2 * runs,)), dma((2 * runs,)), dma((2,)), dma, dma((tiles,)), dma((tiles,)),
        ],
        compiler_params=pltpu.CompilerParams(collective_id=0, has_side_effects=True, vmem_limit_bytes=63 * 2**20),
    )(x, gain, cos, sin, wq, wk, wv, wo)
    return y


def solution(mesh):
    devices = mesh.shape["sp"]

    def step(x, gain, wq, wk, wv, wo):
        own = x.shape[0]
        first = (lax.axis_index("sp") // 2) * 2 * own
        half = HEAD // 2
        angle = (first + jnp.arange(2 * own)).astype(jnp.float32)[:, None] * THETA ** (-jnp.arange(half, dtype=jnp.float32) / half)
        cos, sin = jnp.cos(angle), jnp.sin(angle)
        return layer(x, gain.astype(jnp.float32)[None], jnp.concatenate([cos, cos], -1), jnp.concatenate([-sin, sin], -1), wq, wk, wv, wo, devices // 2)

    tokens, whole = P(("dp", "sp"), None), P(None, None)
    return jax.shard_map(step, mesh=mesh, in_specs=(tokens, P(None), whole, whole, whole, whole), out_specs=tokens, check_vma=False)
```

```python
import functools

import jax
import jax.numpy as jnp
from jax import lax
from jax.experimental import pallas as pl
from jax.experimental.pallas import tpu as pltpu
from jax.sharding import PartitionSpec as P

HEAD = 128
THETA = 10000
HIDDEN = -2e30
LOG2E = 1.4426950408889634
TN = 512
CHUNKS = 4
STRIP = 2
MESH = pl.DeviceIdType.MESH


def _dot(a, b, ca, cb):
    return lax.dot_general(a, b, (((ca,), (cb,)), ((), ())), preferred_element_type=jnp.float32)


def _columns(n, i):
    return pl.ds(pl.multiple_of(i * n, n), n)


def _attend(n, queries, k_s, v_s, put, sent, s_refs, top_refs, mix_refs, own, per, total):
    e = HEAD**-0.5 * LOG2E
    cols = STRIP * own

    def scores(h, b):
        g = lax.div(h, per)
        q = queries(h)
        top = None
        for j in range(n):
            s = _dot(k_s[g, j * own : (j + 1) * own, :], q, 1, 1)
            if j == n - 1:
                ok = lax.rem(lax.broadcasted_iota(jnp.int32, (own, cols), 1), own) >= lax.broadcasted_iota(jnp.int32, (own, cols), 0)
                s = jnp.where(ok, s, HIDDEN)
            s_refs[b][j * own : (j + 1) * own, :] = s
            m = s.reshape(own // 8, 8, cols).max(axis=0)
            top = m if top is None else jnp.maximum(top, m)
            yield
        top_refs[b][...] = jnp.broadcast_to(top.max(axis=0, keepdims=True), (8, cols))

    def mix(h, b):
        g = lax.div(h, per)
        top = top_refs[b][0:1, :]
        acc = None
        for j in range(n):
            here = slice(j * own, (j + 1) * own)
            p = jnp.exp2((s_refs[b][here, :] - top) * e).astype(jnp.bfloat16)
            r = _dot(jnp.concatenate([v_s[g, :, here], jnp.ones((8, own), jnp.bfloat16)], axis=0), p, 1, 0)
            acc = r if acc is None else acc + r
            yield
        mix_refs[b][...] = acc

    def finish(h, b):
        for w in range(STRIP):
            at = slice(w * own, (w + 1) * own)
            put(h * STRIP + w, (mix_refs[b][:HEAD, at] * (1 / mix_refs[b][HEAD : HEAD + 1, at])).T.astype(jnp.bfloat16))

    def side_by_side(*stages):
        stages = list(stages)
        while stages:
            stages = [s for s in stages if next(s, stages) is not stages]

    def pair(i, _):
        finish(2 * i - 2, 0)
        side_by_side(scores(2 * i, 0), mix(2 * i - 1, 1))
        finish(2 * i - 1, 1)
        side_by_side(scores(2 * i + 1, 1), mix(2 * i, 0))
        sent(2 * i)

    side_by_side(scores(0, 0))
    side_by_side(scores(1, 1), mix(0, 0))
    lax.fori_loop(1, total // 2, pair, None)
    finish(total - 2, 0)
    side_by_side(mix(total - 1, 1))
    finish(total - 1, 1)
    sent(total)


def _layer(chips, x_ref, gain_ref, cos_ref, sin_ref, wq_ref, wk_ref, wv_ref, wo_ref, y_ref, far_ref,
           a_s, w_s, k_s, v_s, q_s, s0_s, s1_s, top0_s, top1_s, mix0_s, mix1_s, acc_s, xs_s, ys_s,
           x_sem, a_send, a_recv, far_send, far_recv, w_sem, kv_send, kv_recv, free_sem, s_send, s_recv, xs_sem, y_sem, y_send, y_recv):
    me = lax.axis_index("sp")
    core = lax.rem(me, 2)
    chip = lax.div(me, 2)
    partner = me + 1 - 2 * core
    own, depth = x_ref.shape
    rows = own // CHUNKS
    heads = TN // HEAD
    tiles = depth // 2 // TN
    groups = k_s.shape[0]
    others = [lax.rem(chip + i, chips) * 2 + core for i in range(1, chips)]

    def remote(src, dst, send, recv, device):
        return pltpu.make_async_remote_copy(src, dst, send, recv, device_id={"sp": device}, device_id_type=MESH)

    x_in = [pltpu.make_async_copy(x_ref.at[pl.ds(i * rows, rows)], a_s.at[core, pl.ds(i * rows, rows)], x_sem.at[i]) for i in range(CHUNKS)]
    for c in x_in:
        c.start()

    def weights(ref, i, slot):
        return pltpu.make_async_copy(ref.at[:, _columns(TN, i)], w_s.at[slot], w_sem.at[slot])

    weights(wk_ref, core, 0).start()
    weights(wv_ref, core, 1).start()

    barrier = pltpu.get_barrier_semaphore()
    for d in [partner, *others]:
        pl.semaphore_signal(barrier, inc=1, device_id={"sp": d}, device_id_type=MESH)
    pl.semaphore_wait(barrier, len(others) + 1)

    def share(i, half):
        part = a_s.at[half, pl.ds(i * rows, rows)]
        return remote(part, part, a_send.at[i], a_recv.at[i], partner)

    step = 16

    def norm(i, _):
        here = pl.ds(pl.multiple_of(i * step, step), step)
        wide = a_s[core, here, :].astype(jnp.float32)
        scale = lax.rsqrt(jnp.mean(wide * wide, -1, keepdims=True) + 1e-6)
        a_s[core, here, :] = (wide * scale * gain_ref[...]).astype(jnp.bfloat16)

    for i in range(CHUNKS):
        x_in[i].wait()
        lax.fori_loop(i * rows // step, (i + 1) * rows // step, norm, None)
        share(i, core).start()

    far = remote(x_ref.at[:, _columns(depth // 2, 1 - core)], far_ref, far_send, far_recv, partner)
    far.start()

    def spread(i, kind):
        part = k_s.at[:, _columns(2 * own, chip), :] if kind == 0 else v_s.at[:, :, _columns(2 * own, chip)]
        return remote(part, part, kv_send.at[kind, i], kv_recv.at[kind, i], others[i])

    def turn(one, cos, sin):
        one = one.astype(jnp.bfloat16).astype(jnp.float32)
        return (one * cos + pltpu.roll(one, HEAD // 2, 1) * sin).astype(jnp.bfloat16)

    def keys(j, _):
        slot = lax.rem(j, 2)
        half = jnp.where(j < 2, core, 1 - core)

        @pl.when(j < 2)
        def _():
            weights(wk_ref, 0, slot).wait()

        @pl.when(j == 2)
        def _():
            for i in range(CHUNKS):
                share(i, 1 - core).wait_recv()

        acc_s[:own, :] = _dot(a_s[half], w_s[slot], 1, 0)
        place = _columns(own, chip * 2 + half)

        @pl.when(slot == 0)
        def _():
            at = _columns(own, half)
            for h in range(heads):
                k_s[h, place, :] = turn(acc_s[:own, h * HEAD : (h + 1) * HEAD], cos_ref[at, :], sin_ref[at, :])

        @pl.when(slot == 1)
        def _():
            for h in range(heads):
                v_s[h, :, place] = acc_s[:own, h * HEAD : (h + 1) * HEAD].T.astype(jnp.bfloat16)

        @pl.when(j >= 2)
        def _():
            weights(wq_ref, core * tiles + slot, slot).start()

    lax.fori_loop(0, 4, keys, None)
    for kind in range(2):
        for i in range(len(others)):
            spread(i, kind).start()

    def turn_tile(t):
        for h in range(heads):
            q_s[t * heads + h] = turn(acc_s[:, h * HEAD : (h + 1) * HEAD], cos_ref[...], sin_ref[...])

    def tokens():
        return a_s[...].reshape(2 * own, depth)

    def project(t, _):
        slot = lax.rem(t, 2)
        weights(wq_ref, 0, slot).wait()
        turn_tile(jnp.maximum(t - 1, 0))
        acc_s[...] = _dot(tokens(), w_s[slot], 1, 0)

        @pl.when(t + 2 < tiles)
        def _():
            weights(wq_ref, core * tiles + t + 2, slot).start()

        @pl.when(t + 2 >= tiles)
        def _():
            weights(wo_ref, core * tiles + t + 2 - tiles, slot).start()

    lax.fori_loop(0, tiles, project, None)
    turn_tile(tiles - 1)
    for i in range(CHUNKS):
        share(i, core).wait_send()
    pl.semaphore_signal(free_sem, inc=1, device_id={"sp": partner}, device_id_type=MESH)
    for kind in range(2):
        for i in range(len(others)):
            spread(i, kind).wait()
    pl.semaphore_wait(free_sem, 1)

    query_heads = q_s.shape[0]
    per = query_heads // groups

    def seen(c, g, half):
        part = a_s.at[half, :, _columns(per * HEAD, c * groups + g)]
        return remote(part, part, s_send.at[half, g], s_recv.at[half, g], partner)

    for half in range(2):
        def queries(h, half=half):
            return q_s[pl.ds(h * STRIP, STRIP), half * own : (half + 1) * own, :].reshape(STRIP * own, HEAD)

        def put(h, value, half=half):
            a_s[half, :, _columns(HEAD, core * query_heads + h)] = value

        def sent(h, half=half):
            if isinstance(h, int):
                seen(core, groups - 1, half).start()
            else:
                @pl.when(lax.rem(h * STRIP, per) == 0)
                def _():
                    seen(core, lax.div(h * STRIP, per) - 1, half).start()

        for c in range(chips):
            @pl.when(chip == c)
            def _(c=c):
                _attend(2 * c + half + 1, queries, k_s, v_s, put, sent, (s0_s, s1_s), (top0_s, top1_s), (mix0_s, mix1_s), own, per // STRIP, query_heads // STRIP)

    def residual(t, u):
        half, part = ((1 - core, far_ref.at[:, _columns(TN, t)]), (core, x_ref.at[:, _columns(TN, core * tiles + t)]))[u]
        slot = lax.rem(t, 2)
        return pltpu.make_async_copy(part, xs_s.at[slot, half], xs_sem.at[slot, u])

    def give(c, t):
        return remote(ys_s.at[1 - core], y_ref.at[:, _columns(TN, c * tiles + t)], y_send.at[t], y_recv.at[t], partner)

    def store(t):
        return pltpu.make_async_copy(ys_s.at[core], y_ref.at[:, _columns(TN, core * tiles + t)], y_sem)

    far.wait()
    for half in range(2):
        for g in range(groups):
            seen(1 - core, g, half).wait_recv()

    def ready(t):
        for u in range(2):
            residual(t, u).wait()

        @pl.when(t > 0)
        def _():
            give(core, t - 1).wait_send()
            store(t - 1).wait()

    def add(slot):
        for half in range(2):
            ys_s[half] = (xs_s[slot, half].astype(jnp.float32) + acc_s[half * own : (half + 1) * own, :]).astype(jnp.bfloat16)

    def out(t, _):
        slot = lax.rem(tiles + t, 2)
        weights(wo_ref, 0, slot).wait()
        for u in range(2):
            residual(t, u).start()

        @pl.when(t > 0)
        def _():
            ready(t - 1)

        add(lax.rem(t + 1, 2))
        acc_s[...] = _dot(tokens(), w_s[slot], 1, 0)

        @pl.when(t > 0)
        def _():
            give(core, t - 1).start()
            store(t - 1).start()

        @pl.when(t + 2 < tiles)
        def _():
            weights(wo_ref, core * tiles + t + 2, slot).start()

    lax.fori_loop(0, tiles, out, None)
    ready(tiles - 1)
    add((tiles - 1) % 2)
    give(core, tiles - 1).start()
    store(tiles - 1).start()
    for half in range(2):
        for g in range(groups):
            seen(core, g, half).wait_send()
    give(core, tiles - 1).wait_send()
    store(tiles - 1).wait()
    for t in range(tiles):
        give(1 - core, t).wait_recv()


def layer(x, gain, cos, sin, wq, wk, wv, wo, chips):
    own, depth = x.shape
    heads, kv = wq.shape[1] // HEAD // 2, wk.shape[1] // HEAD // 2
    tiles = depth // 2 // TN
    hbm, vmem = pl.BlockSpec(memory_space=pl.ANY), pl.BlockSpec(memory_space=pltpu.VMEM)
    low, dma = jnp.bfloat16, pltpu.SemaphoreType.DMA
    keys, cols = chips * 2 * own, STRIP * own
    y, _ = pl.pallas_call(
        functools.partial(_layer, chips),
        in_specs=[hbm, vmem, vmem, vmem, hbm, hbm, hbm, hbm],
        out_specs=[hbm, hbm],
        out_shape=[jax.ShapeDtypeStruct((own, depth), low), jax.ShapeDtypeStruct((own, depth // 2), low)],
        scratch_shapes=[
            pltpu.VMEM((2, own, depth), low),
            pltpu.VMEM((2, depth, TN), low),
            pltpu.VMEM((kv, keys, HEAD), low),
            pltpu.VMEM((kv, HEAD, keys), low),
            pltpu.VMEM((heads, 2 * own, HEAD), low),
            pltpu.VMEM((keys, cols), jnp.float32),
            pltpu.VMEM((keys, cols), jnp.float32),
            pltpu.VMEM((8, cols), jnp.float32),
            pltpu.VMEM((8, cols), jnp.float32),
            pltpu.VMEM((HEAD + 8, cols), jnp.float32),
            pltpu.VMEM((HEAD + 8, cols), jnp.float32),
            pltpu.VMEM((2 * own, TN), jnp.float32),
            pltpu.VMEM((2, 2, own, TN), low),
            pltpu.VMEM((2, own, TN), low),
            dma((CHUNKS,)), dma((CHUNKS,)), dma((CHUNKS,)), dma, dma, dma((2,)), dma((2, chips - 1)), dma((2, chips - 1)),
            pltpu.SemaphoreType.REGULAR, dma((2, kv)), dma((2, kv)), dma((2, 2)), dma, dma((tiles,)), dma((tiles,)),
        ],
        compiler_params=pltpu.CompilerParams(collective_id=0, has_side_effects=True, vmem_limit_bytes=63 * 2**20),
    )(x, gain, cos, sin, wq, wk, wv, wo)
    return y


def solution(mesh):
    devices = mesh.shape["sp"]

    def step(x, gain, wq, wk, wv, wo):
        own = x.shape[0]
        first = (lax.axis_index("sp") // 2) * 2 * own
        half = HEAD // 2
        angle = (first + jnp.arange(2 * own)).astype(jnp.float32)[:, None] * THETA ** (-jnp.arange(half, dtype=jnp.float32) / half)
        cos, sin = jnp.cos(angle), jnp.sin(angle)
        return layer(x, gain.astype(jnp.float32)[None], jnp.concatenate([cos, cos], -1), jnp.concatenate([-sin, sin], -1), wq, wk, wv, wo, devices // 2)

    tokens, whole = P(("dp", "sp"), None), P(None, None)
    return jax.shard_map(step, mesh=mesh, in_specs=(tokens, P(None), whole, whole, whole, whole), out_specs=tokens, check_vma=False)
```

```python
import functools

import jax
import jax.numpy as jnp
from jax import lax
from jax.experimental import pallas as pl
from jax.experimental.pallas import tpu as pltpu
from jax.sharding import PartitionSpec as P

HEAD = 128
THETA = 10000
HIDDEN = -2e30
LOG2E = 1.4426950408889634
TN = 512
CHUNKS = 4
STRIP = 2
MESH = pl.DeviceIdType.MESH


def _dot(a, b, ca, cb):
    return lax.dot_general(a, b, (((ca,), (cb,)), ((), ())), preferred_element_type=jnp.float32)


def _columns(n, i):
    return pl.ds(pl.multiple_of(i * n, n), n)


def _attend(n, queries, k_s, v_s, put, sent, s_refs, top_refs, mix_refs, own, per, total):
    e = HEAD**-0.5 * LOG2E
    cols = STRIP * own

    def scores(h, b):
        g = lax.div(h, per)
        q = queries(h)
        top = None
        for j in range(n):
            s = _dot(k_s[g, j * own : (j + 1) * own, :], q, 1, 1)
            if j == n - 1:
                ok = lax.rem(lax.broadcasted_iota(jnp.int32, (own, cols), 1), own) >= lax.broadcasted_iota(jnp.int32, (own, cols), 0)
                s = jnp.where(ok, s, HIDDEN)
            s_refs[b][j * own : (j + 1) * own, :] = s
            m = s.reshape(own // 8, 8, cols).max(axis=0)
            top = m if top is None else jnp.maximum(top, m)
            yield
        top_refs[b][...] = jnp.broadcast_to(top.max(axis=0, keepdims=True), (8, cols))

    def mix(h, b):
        g = lax.div(h, per)
        top = top_refs[b][0:1, :]
        acc = None
        for j in range(n):
            here = slice(j * own, (j + 1) * own)
            p = jnp.exp2((s_refs[b][here, :] - top) * e).astype(jnp.bfloat16)
            r = _dot(jnp.concatenate([v_s[g, :, here], jnp.ones((8, own), jnp.bfloat16)], axis=0), p, 1, 0)
            acc = r if acc is None else acc + r
            yield
        mix_refs[b][...] = acc

    def finish(h, b):
        for w in range(STRIP):
            at = slice(w * own, (w + 1) * own)
            put(h * STRIP + w, (mix_refs[b][:HEAD, at] * (1 / mix_refs[b][HEAD : HEAD + 1, at])).T.astype(jnp.bfloat16))

    def side_by_side(*stages):
        stages = list(stages)
        while stages:
            stages = [s for s in stages if next(s, stages) is not stages]

    def pair(i, _):
        finish(2 * i - 2, 0)
        side_by_side(scores(2 * i, 0), mix(2 * i - 1, 1))
        finish(2 * i - 1, 1)
        side_by_side(scores(2 * i + 1, 1), mix(2 * i, 0))
        sent(2 * i)

    side_by_side(scores(0, 0))
    side_by_side(scores(1, 1), mix(0, 0))
    lax.fori_loop(1, total // 2, pair, None)
    finish(total - 2, 0)
    side_by_side(mix(total - 1, 1))
    finish(total - 1, 1)
    sent(total)


def _layer(chips, x_ref, gain_ref, rate_ref, wq_ref, wk_ref, wv_ref, wo_ref, y_ref, far_ref,
           a_s, w_s, k_s, v_s, q_s, cos_ref, sin_ref, s0_s, s1_s, top0_s, top1_s, mix0_s, mix1_s, acc_s, xs_s, ys_s,
           x_sem, a_send, a_recv, far_send, far_recv, w_sem, kv_send, kv_recv, free_sem, s_send, s_recv, xs_sem, y_sem, y_send, y_recv):
    me = lax.axis_index("sp")
    core = lax.rem(me, 2)
    chip = lax.div(me, 2)
    partner = me + 1 - 2 * core
    own, depth = x_ref.shape
    rows = own // CHUNKS
    heads = TN // HEAD
    tiles = depth // 2 // TN
    groups = k_s.shape[0]
    others = [lax.rem(chip + i, chips) * 2 + core for i in range(1, chips)]

    def remote(src, dst, send, recv, device):
        return pltpu.make_async_remote_copy(src, dst, send, recv, device_id={"sp": device}, device_id_type=MESH)

    x_in = [pltpu.make_async_copy(x_ref.at[pl.ds(i * rows, rows)], a_s.at[core, pl.ds(i * rows, rows)], x_sem.at[i]) for i in range(CHUNKS)]
    for c in x_in:
        c.start()

    def weights(ref, i, slot):
        return pltpu.make_async_copy(ref.at[:, _columns(TN, i)], w_s.at[slot], w_sem.at[slot])

    weights(wk_ref, core, 0).start()
    weights(wv_ref, core, 1).start()

    def table(i, _):
        block = (32, HEAD)
        here = _columns(block[0], i)
        place = (lax.broadcasted_iota(jnp.int32, block, 0) + (chip * 2 * own + i * block[0])).astype(jnp.float32)
        angle = place * rate_ref[...]
        cos_ref[here, :] = jnp.cos(angle)
        sin_ref[here, :] = jnp.where(lax.broadcasted_iota(jnp.int32, block, 1) < HEAD // 2, -1.0, 1.0) * jnp.sin(angle)

    lax.fori_loop(0, 2 * own // 32, table, None)

    barrier = pltpu.get_barrier_semaphore()
    for d in [partner, *others]:
        pl.semaphore_signal(barrier, inc=1, device_id={"sp": d}, device_id_type=MESH)
    pl.semaphore_wait(barrier, len(others) + 1)

    def share(i, half):
        part = a_s.at[half, pl.ds(i * rows, rows)]
        return remote(part, part, a_send.at[i], a_recv.at[i], partner)

    step = 16

    def norm(i, _):
        here = pl.ds(pl.multiple_of(i * step, step), step)
        wide = a_s[core, here, :].astype(jnp.float32)
        scale = lax.rsqrt(jnp.mean(wide * wide, -1, keepdims=True) + 1e-6)
        a_s[core, here, :] = (wide * scale * gain_ref[...].astype(jnp.float32)).astype(jnp.bfloat16)

    for i in range(CHUNKS):
        x_in[i].wait()
        lax.fori_loop(i * rows // step, (i + 1) * rows // step, norm, None)
        share(i, core).start()

    far = remote(x_ref.at[:, _columns(depth // 2, 1 - core)], far_ref, far_send, far_recv, partner)
    far.start()

    def spread(i, kind):
        part = k_s.at[:, _columns(2 * own, chip), :] if kind == 0 else v_s.at[:, :, _columns(2 * own, chip)]
        return remote(part, part, kv_send.at[kind, i], kv_recv.at[kind, i], others[i])

    def turn(one, cos, sin):
        one = one.astype(jnp.bfloat16).astype(jnp.float32)
        return (one * cos + pltpu.roll(one, HEAD // 2, 1) * sin).astype(jnp.bfloat16)

    def keys(j, _):
        slot = lax.rem(j, 2)
        half = jnp.where(j < 2, core, 1 - core)

        @pl.when(j < 2)
        def _():
            weights(wk_ref, 0, slot).wait()

        @pl.when(j == 2)
        def _():
            for i in range(CHUNKS):
                share(i, 1 - core).wait_recv()

        acc_s[:own, :] = _dot(a_s[half], w_s[slot], 1, 0)
        place = _columns(own, chip * 2 + half)

        @pl.when(slot == 0)
        def _():
            at = _columns(own, half)
            for h in range(heads):
                k_s[h, place, :] = turn(acc_s[:own, h * HEAD : (h + 1) * HEAD], cos_ref[at, :], sin_ref[at, :])

        @pl.when(slot == 1)
        def _():
            for h in range(heads):
                v_s[h, :, place] = acc_s[:own, h * HEAD : (h + 1) * HEAD].T.astype(jnp.bfloat16)

        @pl.when(j >= 2)
        def _():
            weights(wq_ref, core * tiles + slot, slot).start()

    lax.fori_loop(0, 4, keys, None)
    for kind in range(2):
        for i in range(len(others)):
            spread(i, kind).start()

    def turn_tile(t):
        for h in range(heads):
            q_s[t * heads + h] = turn(acc_s[:, h * HEAD : (h + 1) * HEAD], cos_ref[...], sin_ref[...])

    def tokens():
        return a_s[...].reshape(2 * own, depth)

    def project(t, _):
        slot = lax.rem(t, 2)
        weights(wq_ref, 0, slot).wait()
        turn_tile(jnp.maximum(t - 1, 0))
        acc_s[...] = _dot(tokens(), w_s[slot], 1, 0)

        @pl.when(t + 2 < tiles)
        def _():
            weights(wq_ref, core * tiles + t + 2, slot).start()

        @pl.when(t + 2 >= tiles)
        def _():
            weights(wo_ref, core * tiles + t + 2 - tiles, slot).start()

    lax.fori_loop(0, tiles, project, None)
    turn_tile(tiles - 1)
    for i in range(CHUNKS):
        share(i, core).wait_send()
    pl.semaphore_signal(free_sem, inc=1, device_id={"sp": partner}, device_id_type=MESH)
    for kind in range(2):
        for i in range(len(others)):
            spread(i, kind).wait()
    pl.semaphore_wait(free_sem, 1)

    query_heads = q_s.shape[0]
    per = query_heads // groups

    def seen(c, g, half):
        part = a_s.at[half, :, _columns(per * HEAD, c * groups + g)]
        return remote(part, part, s_send.at[half, g], s_recv.at[half, g], partner)

    for half in range(2):
        def queries(h, half=half):
            return q_s[pl.ds(h * STRIP, STRIP), half * own : (half + 1) * own, :].reshape(STRIP * own, HEAD)

        def put(h, value, half=half):
            a_s[half, :, _columns(HEAD, core * query_heads + h)] = value

        def sent(h, half=half):
            if isinstance(h, int):
                seen(core, groups - 1, half).start()
            else:
                @pl.when(lax.rem(h * STRIP, per) == 0)
                def _():
                    seen(core, lax.div(h * STRIP, per) - 1, half).start()

        for c in range(chips):
            @pl.when(chip == c)
            def _(c=c):
                _attend(2 * c + half + 1, queries, k_s, v_s, put, sent, (s0_s, s1_s), (top0_s, top1_s), (mix0_s, mix1_s), own, per // STRIP, query_heads // STRIP)

    def residual(t, u):
        half, part = ((1 - core, far_ref.at[:, _columns(TN, t)]), (core, x_ref.at[:, _columns(TN, core * tiles + t)]))[u]
        slot = lax.rem(t, 2)
        return pltpu.make_async_copy(part, xs_s.at[slot, half], xs_sem.at[slot, u])

    def give(c, t):
        return remote(ys_s.at[lax.rem(t, 2), 1 - core], y_ref.at[:, _columns(TN, c * tiles + t)], y_send.at[t], y_recv.at[t], partner)

    def store(t):
        slot = lax.rem(t, 2)
        return pltpu.make_async_copy(ys_s.at[slot, core], y_ref.at[:, _columns(TN, core * tiles + t)], y_sem.at[slot])

    far.wait()
    for half in range(2):
        for g in range(groups):
            seen(1 - core, g, half).wait_recv()

    def ready(t):
        for u in range(2):
            residual(t, u).wait()

        @pl.when(t >= 2)
        def _():
            give(core, t - 2).wait_send()
            store(t - 2).wait()

    def add(slot):
        for half in range(2):
            ys_s[slot, half] = (xs_s[slot, half].astype(jnp.float32) + acc_s[half * own : (half + 1) * own, :]).astype(jnp.bfloat16)

    def out(t, _):
        slot = lax.rem(tiles + t, 2)
        weights(wo_ref, 0, slot).wait()
        for u in range(2):
            residual(t, u).start()

        @pl.when(t > 0)
        def _():
            ready(t - 1)

        add(lax.rem(t + 1, 2))
        acc_s[...] = _dot(tokens(), w_s[slot], 1, 0)

        @pl.when(t > 0)
        def _():
            give(core, t - 1).start()
            store(t - 1).start()

        @pl.when(t + 2 < tiles)
        def _():
            weights(wo_ref, core * tiles + t + 2, slot).start()

    lax.fori_loop(0, tiles, out, None)
    ready(tiles - 1)
    add((tiles - 1) % 2)
    give(core, tiles - 1).start()
    store(tiles - 1).start()
    for half in range(2):
        for g in range(groups):
            seen(core, g, half).wait_send()
    for t in (tiles - 2, tiles - 1):
        give(core, t).wait_send()
        store(t).wait()
    for t in range(tiles):
        give(1 - core, t).wait_recv()


def layer(x, gain, rate, wq, wk, wv, wo, chips):
    own, depth = x.shape
    heads, kv = wq.shape[1] // HEAD // 2, wk.shape[1] // HEAD // 2
    tiles = depth // 2 // TN
    hbm, vmem = pl.BlockSpec(memory_space=pl.ANY), pl.BlockSpec(memory_space=pltpu.VMEM)
    low, dma = jnp.bfloat16, pltpu.SemaphoreType.DMA
    keys, cols = chips * 2 * own, STRIP * own
    y, _ = pl.pallas_call(
        functools.partial(_layer, chips),
        in_specs=[hbm, vmem, vmem, hbm, hbm, hbm, hbm],
        out_specs=[hbm, hbm],
        out_shape=[jax.ShapeDtypeStruct((own, depth), low), jax.ShapeDtypeStruct((own, depth // 2), low)],
        scratch_shapes=[
            pltpu.VMEM((2, own, depth), low),
            pltpu.VMEM((2, depth, TN), low),
            pltpu.VMEM((kv, keys, HEAD), low),
            pltpu.VMEM((kv, HEAD, keys), low),
            pltpu.VMEM((heads, 2 * own, HEAD), low),
            pltpu.VMEM((2 * own, HEAD), jnp.float32),
            pltpu.VMEM((2 * own, HEAD), jnp.float32),
            pltpu.VMEM((keys, cols), jnp.float32),
            pltpu.VMEM((keys, cols), jnp.float32),
            pltpu.VMEM((8, cols), jnp.float32),
            pltpu.VMEM((8, cols), jnp.float32),
            pltpu.VMEM((HEAD + 8, cols), jnp.float32),
            pltpu.VMEM((HEAD + 8, cols), jnp.float32),
            pltpu.VMEM((2 * own, TN), jnp.float32),
            pltpu.VMEM((2, 2, own, TN), low),
            pltpu.VMEM((2, 2, own, TN), low),
            dma((CHUNKS,)), dma((CHUNKS,)), dma((CHUNKS,)), dma, dma, dma((2,)), dma((2, chips - 1)), dma((2, chips - 1)),
            pltpu.SemaphoreType.REGULAR, dma((2, kv)), dma((2, kv)), dma((2, 2)), dma((2,)), dma((tiles,)), dma((tiles,)),
        ],
        compiler_params=pltpu.CompilerParams(collective_id=0, has_side_effects=True, vmem_limit_bytes=67043328),
    )(x, gain, rate, wq, wk, wv, wo)
    return y


def solution(mesh):
    devices = mesh.shape["sp"]

    def step(x, gain, wq, wk, wv, wo):
        half = HEAD // 2
        rate = THETA ** (-jnp.arange(half, dtype=jnp.float32) / half)
        return layer(x, gain[None], jnp.concatenate([rate, rate])[None], wq, wk, wv, wo, devices // 2)

    tokens, whole = P(("dp", "sp"), None), P(None, None)
    return jax.shard_map(step, mesh=mesh, in_specs=(tokens, P(None), whole, whole, whole, whole), out_specs=tokens, check_vma=False)
```

```python
import functools

import jax
import jax.numpy as jnp
import numpy as np
from jax import lax
from jax.experimental import pallas as pl
from jax.experimental.pallas import tpu as pltpu
from jax.sharding import PartitionSpec as P

HEAD = 128
THETA = 10000
HIDDEN = -2e30
LOG2E = 1.4426950408889634
TN = 512
CHUNKS = 4
STRIP = 2
MESH = pl.DeviceIdType.MESH


def _dot(a, b, ca, cb):
    return lax.dot_general(a, b, (((ca,), (cb,)), ((), ())), preferred_element_type=jnp.float32)


def _columns(n, i):
    return pl.ds(pl.multiple_of(i * n, n), n)


def _attend(n, queries, k_s, v_s, put, sent, s_refs, top_refs, mix_refs, own, per, total):
    e = HEAD**-0.5 * LOG2E
    cols = STRIP * own

    def scores(h, b):
        g = lax.div(h, per)
        q = queries(h)
        top = None
        for j in range(n):
            s = _dot(k_s[g, j * own : (j + 1) * own, :], q, 1, 1)
            if j == n - 1:
                ok = lax.rem(lax.broadcasted_iota(jnp.int32, (own, cols), 1), own) >= lax.broadcasted_iota(jnp.int32, (own, cols), 0)
                s = jnp.where(ok, s, HIDDEN)
            s_refs[b][j * own : (j + 1) * own, :] = s
            m = s.reshape(own // 8, 8, cols).max(axis=0)
            top = m if top is None else jnp.maximum(top, m)
            yield
        top_refs[b][...] = jnp.broadcast_to(top.max(axis=0, keepdims=True), (8, cols))

    def mix(h, b):
        g = lax.div(h, per)
        top = top_refs[b][0:1, :]
        acc = None
        for j in range(n):
            here = slice(j * own, (j + 1) * own)
            p = jnp.exp2((s_refs[b][here, :] - top) * e).astype(jnp.bfloat16)
            r = _dot(jnp.concatenate([v_s[g, :, here], jnp.ones((8, own), jnp.bfloat16)], axis=0), p, 1, 0)
            acc = r if acc is None else acc + r
            yield
        mix_refs[b][...] = acc

    def finish(h, b):
        for w in range(STRIP):
            at = slice(w * own, (w + 1) * own)
            put(h * STRIP + w, (mix_refs[b][:HEAD, at] * (1 / mix_refs[b][HEAD : HEAD + 1, at])).T.astype(jnp.bfloat16))

    def side_by_side(*stages):
        stages = list(stages)
        while stages:
            stages = [s for s in stages if next(s, stages) is not stages]

    def pair(i, _):
        finish(2 * i - 2, 0)
        side_by_side(scores(2 * i, 0), mix(2 * i - 1, 1))
        finish(2 * i - 1, 1)
        side_by_side(scores(2 * i + 1, 1), mix(2 * i, 0))
        sent(2 * i)

    side_by_side(scores(0, 0))
    side_by_side(scores(1, 1), mix(0, 0))
    lax.fori_loop(1, total // 2, pair, None)
    finish(total - 2, 0)
    side_by_side(mix(total - 1, 1))
    finish(total - 1, 1)
    sent(total)


def _layer(chips, x_ref, gain_ref, rate_ref, wq_ref, wk_ref, wv_ref, wo_ref, y_ref, far_ref,
           a_s, w_s, k_s, v_s, q_s, cos_ref, sin_ref, s0_s, s1_s, top0_s, top1_s, mix0_s, mix1_s, acc_s, xs_s, ys_s,
           x_sem, a_send, a_recv, far_send, far_recv, w_sem, kv_send, kv_recv, free_sem, s_send, s_recv, xs_sem, y_sem, y_send, y_recv):
    me = lax.axis_index("sp")
    core = lax.rem(me, 2)
    chip = lax.div(me, 2)
    partner = me + 1 - 2 * core
    own, depth = x_ref.shape
    rows = own // CHUNKS
    heads = TN // HEAD
    tiles = depth // 2 // TN
    groups = k_s.shape[0]
    others = [lax.rem(chip + i, chips) * 2 + core for i in range(1, chips)]

    def remote(src, dst, send, recv, device):
        return pltpu.make_async_remote_copy(src, dst, send, recv, device_id={"sp": device}, device_id_type=MESH)

    x_in = [pltpu.make_async_copy(x_ref.at[pl.ds(i * rows, rows)], a_s.at[core, pl.ds(i * rows, rows)], x_sem.at[i]) for i in range(CHUNKS)]
    for c in x_in:
        c.start()

    def weights(ref, i, slot):
        return pltpu.make_async_copy(ref.at[:, _columns(TN, i)], w_s.at[slot], w_sem.at[slot])

    weights(wk_ref, core, 0).start()
    weights(wv_ref, core, 1).start()

    def table(i, _):
        block = (32, HEAD)
        here = _columns(block[0], i)
        place = (lax.broadcasted_iota(jnp.int32, block, 0) + (chip * 2 * own + i * block[0])).astype(jnp.float32)
        angle = place * rate_ref[...]
        cos_ref[here, :] = jnp.cos(angle)
        sin_ref[here, :] = jnp.where(lax.broadcasted_iota(jnp.int32, block, 1) < HEAD // 2, -1.0, 1.0) * jnp.sin(angle)

    lax.fori_loop(0, 2 * own // 32, table, None)

    barrier = pltpu.get_barrier_semaphore()
    for d in [partner, *others]:
        pl.semaphore_signal(barrier, inc=1, device_id={"sp": d}, device_id_type=MESH)
    pl.semaphore_wait(barrier, len(others) + 1)

    def share(i, half):
        part = a_s.at[half, pl.ds(i * rows, rows)]
        return remote(part, part, a_send.at[i], a_recv.at[i], partner)

    step = 32

    def norm(i, _):
        here = pl.ds(pl.multiple_of(i * step, step), step)
        wide = a_s[core, here, :].astype(jnp.float32)
        scale = lax.rsqrt(jnp.mean(wide * wide, -1, keepdims=True) + 1e-6)
        a_s[core, here, :] = (wide * scale * gain_ref[...].astype(jnp.float32)).astype(jnp.bfloat16)

    for i in range(CHUNKS):
        x_in[i].wait()
        lax.fori_loop(i * rows // step, (i + 1) * rows // step, norm, None)
        share(i, core).start()

    far = remote(x_ref.at[:, _columns(depth // 2, 1 - core)], far_ref, far_send, far_recv, partner)
    far.start()

    def spread(i, kind):
        part = k_s.at[:, _columns(2 * own, chip), :] if kind == 0 else v_s.at[:, :, _columns(2 * own, chip)]
        return remote(part, part, kv_send.at[kind, i], kv_recv.at[kind, i], others[i])

    def turn(one, cos, sin):
        one = one.astype(jnp.bfloat16).astype(jnp.float32)
        return (one * cos + pltpu.roll(one, HEAD // 2, 1) * sin).astype(jnp.bfloat16)

    def keys(j, _):
        slot = lax.rem(j, 2)
        half = jnp.where(j < 2, core, 1 - core)

        @pl.when(j < 2)
        def _():
            weights(wk_ref, 0, slot).wait()

        @pl.when(j == 2)
        def _():
            for i in range(CHUNKS):
                share(i, 1 - core).wait_recv()

        acc_s[:own, :] = _dot(a_s[half], w_s[slot], 1, 0)
        place = _columns(own, chip * 2 + half)

        @pl.when(slot == 0)
        def _():
            at = _columns(own, half)
            for h in range(heads):
                k_s[h, place, :] = turn(acc_s[:own, h * HEAD : (h + 1) * HEAD], cos_ref[at, :], sin_ref[at, :])

        @pl.when(slot == 1)
        def _():
            for h in range(heads):
                v_s[h, :, place] = acc_s[:own, h * HEAD : (h + 1) * HEAD].T.astype(jnp.bfloat16)

        @pl.when(j >= 2)
        def _():
            weights(wq_ref, core * tiles + slot, slot).start()

    lax.fori_loop(0, 4, keys, None)
    for kind in range(2):
        for i in range(len(others)):
            spread(i, kind).start()

    def turn_tile(t):
        for h in range(heads):
            q_s[t * heads + h] = turn(acc_s[:, h * HEAD : (h + 1) * HEAD], cos_ref[...], sin_ref[...])

    def tokens():
        return a_s[...].reshape(2 * own, depth)

    def project(t, _):
        slot = lax.rem(t, 2)
        weights(wq_ref, 0, slot).wait()
        turn_tile(jnp.maximum(t - 1, 0))
        acc_s[...] = _dot(tokens(), w_s[slot], 1, 0)

        @pl.when(t + 2 < tiles)
        def _():
            weights(wq_ref, core * tiles + t + 2, slot).start()

        @pl.when(t + 2 >= tiles)
        def _():
            weights(wo_ref, core * tiles + t + 2 - tiles, slot).start()

    lax.fori_loop(0, tiles, project, None)
    turn_tile(tiles - 1)
    for i in range(CHUNKS):
        share(i, core).wait_send()
    pl.semaphore_signal(free_sem, inc=1, device_id={"sp": partner}, device_id_type=MESH)
    for kind in range(2):
        for i in range(len(others)):
            spread(i, kind).wait()
    pl.semaphore_wait(free_sem, 1)

    query_heads = q_s.shape[0]
    per = query_heads // groups

    def seen(c, g, half):
        part = a_s.at[half, :, _columns(per * HEAD, c * groups + g)]
        return remote(part, part, s_send.at[half, g], s_recv.at[half, g], partner)

    for half in range(2):
        def queries(h, half=half):
            return q_s[pl.ds(h * STRIP, STRIP), half * own : (half + 1) * own, :].reshape(STRIP * own, HEAD)

        def put(h, value, half=half):
            a_s[half, :, _columns(HEAD, core * query_heads + h)] = value

        def sent(h, half=half):
            if isinstance(h, int):
                seen(core, groups - 1, half).start()
            else:
                @pl.when(lax.rem(h * STRIP, per) == 0)
                def _():
                    seen(core, lax.div(h * STRIP, per) - 1, half).start()

        for c in range(chips):
            @pl.when(chip == c)
            def _(c=c):
                _attend(2 * c + half + 1, queries, k_s, v_s, put, sent, (s0_s, s1_s), (top0_s, top1_s), (mix0_s, mix1_s), own, per // STRIP, query_heads // STRIP)

    def residual(t, u):
        half, part = ((1 - core, far_ref.at[:, _columns(TN, t)]), (core, x_ref.at[:, _columns(TN, core * tiles + t)]))[u]
        slot = lax.rem(t, 2)
        return pltpu.make_async_copy(part, xs_s.at[slot, half], xs_sem.at[slot, u])

    def give(c, t):
        return remote(ys_s.at[lax.rem(t, 2), 1 - core], y_ref.at[:, _columns(TN, c * tiles + t)], y_send.at[t], y_recv.at[t], partner)

    def store(t):
        slot = lax.rem(t, 2)
        return pltpu.make_async_copy(ys_s.at[slot, core], y_ref.at[:, _columns(TN, core * tiles + t)], y_sem.at[slot])

    far.wait()
    for half in range(2):
        for g in range(groups):
            seen(1 - core, g, half).wait_recv()

    def ready(t):
        for u in range(2):
            residual(t, u).wait()

        @pl.when(t >= 2)
        def _():
            give(core, t - 2).wait_send()
            store(t - 2).wait()

    def add(slot):
        for half in range(2):
            ys_s[slot, half] = (xs_s[slot, half].astype(jnp.float32) + acc_s[half * own : (half + 1) * own, :]).astype(jnp.bfloat16)

    def out(t, _):
        slot = lax.rem(tiles + t, 2)
        weights(wo_ref, 0, slot).wait()
        for u in range(2):
            residual(t, u).start()

        @pl.when(t > 0)
        def _():
            ready(t - 1)

        add(lax.rem(t + 1, 2))
        acc_s[...] = _dot(tokens(), w_s[slot], 1, 0)

        @pl.when(t > 0)
        def _():
            give(core, t - 1).start()
            store(t - 1).start()

        @pl.when(t + 2 < tiles)
        def _():
            weights(wo_ref, core * tiles + t + 2, slot).start()

    lax.fori_loop(0, tiles, out, None)
    ready(tiles - 1)
    add((tiles - 1) % 2)
    give(core, tiles - 1).start()
    store(tiles - 1).start()
    for half in range(2):
        for g in range(groups):
            seen(core, g, half).wait_send()
    for t in (tiles - 2, tiles - 1):
        give(core, t).wait_send()
        store(t).wait()
    for t in range(tiles):
        give(1 - core, t).wait_recv()


def _moved(parts, src_ref, dst_ref, held_s, in_sem, out_sem):
    rows = src_ref.shape[0] // parts
    at = [pl.ds(i * rows, rows) for i in range(parts)]
    taken = [pltpu.make_async_copy(src_ref.at[at[i]], held_s.at[at[i]], in_sem.at[i]) for i in range(parts)]
    given = [pltpu.make_async_copy(held_s.at[at[i]], dst_ref.at[at[i]], out_sem.at[i]) for i in range(parts)]
    for c in taken:
        c.start()
    for i in range(parts):
        taken[i].wait()
        given[i].start()
    for c in given:
        c.wait()


def moved(y, parts=16):
    hbm, dma = pl.BlockSpec(memory_space=pl.ANY), pltpu.SemaphoreType.DMA
    return pl.pallas_call(
        functools.partial(_moved, parts),
        in_specs=[hbm],
        out_specs=hbm,
        out_shape=jax.ShapeDtypeStruct(y.shape, y.dtype),
        scratch_shapes=[pltpu.VMEM(y.shape, y.dtype), dma((parts,)), dma((parts,))],
        compiler_params=pltpu.CompilerParams(vmem_limit_bytes=67043328),
    )(y)


def layer(x, gain, rate, wq, wk, wv, wo, chips):
    own, depth = x.shape
    heads, kv = wq.shape[1] // HEAD // 2, wk.shape[1] // HEAD // 2
    tiles = depth // 2 // TN
    hbm, vmem = pl.BlockSpec(memory_space=pl.ANY), pl.BlockSpec(memory_space=pltpu.VMEM)
    low, dma = jnp.bfloat16, pltpu.SemaphoreType.DMA
    keys, cols = chips * 2 * own, STRIP * own
    y, _ = pl.pallas_call(
        functools.partial(_layer, chips),
        in_specs=[hbm, vmem, vmem, hbm, hbm, hbm, hbm],
        out_specs=[hbm, hbm],
        out_shape=[jax.ShapeDtypeStruct((own, depth), low), jax.ShapeDtypeStruct((own, depth // 2), low)],
        scratch_shapes=[
            pltpu.VMEM((2, own, depth), low),
            pltpu.VMEM((2, depth, TN), low),
            pltpu.VMEM((kv, keys, HEAD), low),
            pltpu.VMEM((kv, HEAD, keys), low),
            pltpu.VMEM((heads, 2 * own, HEAD), low),
            pltpu.VMEM((2 * own, HEAD), jnp.float32),
            pltpu.VMEM((2 * own, HEAD), jnp.float32),
            pltpu.VMEM((keys, cols), jnp.float32),
            pltpu.VMEM((keys, cols), jnp.float32),
            pltpu.VMEM((8, cols), jnp.float32),
            pltpu.VMEM((8, cols), jnp.float32),
            pltpu.VMEM((HEAD + 8, cols), jnp.float32),
            pltpu.VMEM((HEAD + 8, cols), jnp.float32),
            pltpu.VMEM((2 * own, TN), jnp.float32),
            pltpu.VMEM((2, 2, own, TN), low),
            pltpu.VMEM((2, 2, own, TN), low),
            dma((CHUNKS,)), dma((CHUNKS,)), dma((CHUNKS,)), dma, dma, dma((2,)), dma((2, chips - 1)), dma((2, chips - 1)),
            pltpu.SemaphoreType.REGULAR, dma((2, kv)), dma((2, kv)), dma((2, 2)), dma((2,)), dma((tiles,)), dma((tiles,)),
        ],
        compiler_params=pltpu.CompilerParams(collective_id=0, has_side_effects=True, vmem_limit_bytes=67043328),
    )(x, gain, rate, wq, wk, wv, wo)
    return moved(y)


def solution(mesh):
    devices = mesh.shape["sp"]

    def step(x, gain, wq, wk, wv, wo):
        half = HEAD // 2
        rate = np.float32(float(THETA) ** (-np.arange(half) / half))
        return layer(x, gain[None], jnp.asarray(np.concatenate([rate, rate])[None]), wq, wk, wv, wo, devices // 2)

    tokens, whole = P(("dp", "sp"), None), P(None, None)
    return jax.shard_map(step, mesh=mesh, in_specs=(tokens, P(None), whole, whole, whole, whole), out_specs=tokens, check_vma=False)
```
